32 devices in a mesh: scan: 2 (over y), ang: 4 (over z), row: 4 (over x, core).
Axes of the slice: x: 2, y: 2, z: 4, core: 2. Of those that a mesh axis runs over, the one named last changes fastest.
Arguments:
- projections: bfloat16 [8, 32, 2560], P(('scan', 'ang'), 'row'), parts along dimension 0, may hold values from 0 to 2
- flats: float32 [64, 2560], P(('scan', 'row')), parts along dimension 0, may hold values from 1 to 3
- block_start: int32 [4, 4], replicated, may hold values from 0 to 2528
- bp_weights: bfloat16 [4, 32, 1024], P(None, None, 'ang'), may hold values from -0.5 to 0.5
Outputs:
- recon: float32 [64, 1024], P(('scan', 'row'), 'ang'), parts along dimension 0
The draws below stay inside these ranges and needn't reach their ends.
There are 2 independent parts, one for each index of `scan`. The reference program is written for one: setup_inputs(seed, part) draws one part's arguments, and reference() takes and returns one part's arrays. A program takes and returns all parts, laid end to end along the dimension named above; an argument that names none is the same for every part. Nothing has to cross between parts.
Inputs may be any that keep to these rules, and one draw needn't show every extreme that they name: block_start[a, r] is the first of the 32 detector columns that pixel region r reads at angle a.
All inputs are finite; a program needn't handle non-finite values.
Results may differ from the reference program's by a relative error of at most 0.009.
Values may be sent and summed in bfloat16 or wider, within the bound.
No kernel may reach another device: no remote copies, remote signals or barrier semaphores. Data moves between devices by JAX's collectives and lax.ppermute only.
A program may use at most 64 MiB of HBM per device.

```python
import math
import jax
import jax.numpy as jnp
from jax import lax

W = 2560
RD = 8
HALO = 4
CB = 32
PIX_DEV = 256
TILE = 16
ANGLES = 4
SLICES = 32
REGIONS = 4
PIX = 1024


def set_ends(entries, stream_key, smallest, largest):
    shape = entries.shape
    spot = [jax.random.randint(jax.random.fold_in(stream_key, axis), (), 0, shape[axis]) for axis in range(len(shape))]
    entries = entries.at[tuple(spot)].set(smallest)
    longest = shape.index(max(shape))
    spot[longest] = (spot[longest] + 1) % shape[longest]
    return entries.at[tuple(spot)].set(largest)


def levels(rng, extent, shards, least, largest):
    factor_of = 1.0
    for position, shards_of in shards:
        steps = jax.random.uniform(jax.random.fold_in(jax.random.fold_in(rng, 6), position), (shards_of,), jnp.float32, least / len(shards), largest / len(shards))
        factor_of = factor_of * jnp.repeat(jnp.exp(steps), extent[position] // shards_of).reshape((-1,) + (1,) * (len(extent) - 1 - position))
    return factor_of


def gaussian(own_key, dims, scale, bound, shards=(), kind=jnp.bfloat16):
    array = jax.random.normal(own_key, dims, jnp.float32) * scale
    if len(shards) > 0:
        array = levels(own_key, dims, shards, -0.22, 0.18) * array
    return jnp.clip(array, min=-bound, max=bound).astype(kind)


def setup_inputs(seed: int = 0, part: int = 0) -> dict:
    keys = jax.random.split(jax.random.key(seed), 5)
    part_splits = jax.random.split(jax.random.fold_in(keys[4], part), 5)
    projections = jnp.clip(2.0 * jax.random.uniform(part_splits[0], (ANGLES, SLICES, W), jnp.float32) ** levels(part_splits[0], (ANGLES, SLICES, W), ((0, 4), (1, 4)), -0.2, 0.2), 0.0, 2.0).astype(jnp.bfloat16)
    flats = jnp.clip(jnp.exp(math.log(3.0) - 1.0986123 * jax.random.uniform(part_splits[1], (SLICES, W), jnp.float32) ** levels(part_splits[1], (SLICES, W), ((0, 4),), -0.2, 0.2)), 1.0, 3.0)
    block_start = set_ends(jax.random.randint(keys[2], (ANGLES, REGIONS), 0, W - CB + 1), jax.random.fold_in(keys[2], 1), 0, W - CB).astype(jnp.int32)
    bp_weights = gaussian(keys[3], (ANGLES, CB, PIX), (ANGLES * CB) ** -0.5, 0.5, ((2, 4),))
    return dict(projections=projections, flats=flats, block_start=block_start, bp_weights=bp_weights)


paganin_beta = 8.0
ramp_gain = 320.0


def reference(projections, flats, block_start, bp_weights):
    contrast = 1.0 - projections.astype(jnp.float32) / flats[None, :, :]
    padded = jnp.pad(contrast, ((0, 0), (HALO, HALO), (0, 0)))
    tile_count = SLICES // RD
    row_index = (jnp.arange(tile_count, dtype=jnp.int32)[:, None] * RD
                 + jnp.arange(TILE, dtype=jnp.int32)[None, :]).astype(jnp.int32)
    row_freq = jnp.arange(TILE, dtype=jnp.float32)
    col_freq = jnp.arange(W, dtype=jnp.float32)
    lam = (4.0 * jnp.sin(jnp.pi * row_freq / TILE) ** 2)[:, None] + (4.0 * jnp.sin(jnp.pi * col_freq / W) ** 2)[None, :]
    filt = 1.0 / (1.0 + paganin_beta * lam)
    folded = jnp.minimum(col_freq, W - col_freq)
    ramp = ramp_gain * (folded / W) * (0.5 + 0.5 * jnp.cos(2.0 * jnp.pi * folded / W))

    def one_angle(angle_rows):
        tiles = angle_rows[row_index]
        spectrum = jnp.fft.fft2(tiles, axes=(1, 2)) * filt
        back = jnp.real(jnp.fft.ifft2(spectrum, axes=(1, 2)))
        paganin = back[:, HALO:HALO + RD, :].reshape(SLICES, W)
        filtered = jnp.real(jnp.fft.ifft(jnp.fft.fft(paganin, axis=-1) * ramp, axis=-1))
        return filtered.astype(jnp.bfloat16)

    sinogram = lax.map(one_angle, padded)
    offsets = jnp.arange(CB, dtype=jnp.int32)

    def one_region(region):
        starts = lax.dynamic_index_in_dim(block_start, region, 1, keepdims=False)
        index = (starts[:, None] + offsets[None, :]).astype(jnp.int32)
        index = jnp.broadcast_to(index[:, None, :], (ANGLES, SLICES, CB))
        blocks = jnp.take_along_axis(sinogram, index, axis=2)
        weights = lax.dynamic_slice_in_dim(bp_weights, region * PIX_DEV, PIX_DEV, 2)
        return jnp.einsum('asc,acp->sp', blocks.astype(jnp.float32), weights.astype(jnp.float32))

    parts = lax.map(one_region, jnp.arange(REGIONS, dtype=jnp.int32))
    return jnp.transpose(parts, (1, 0, 2)).reshape(SLICES, PIX)
```

```python
import functools

import jax
import jax.numpy as jnp
import numpy as np
from jax import lax
from jax.experimental import pallas as pl
from jax.experimental.pallas import tpu as pltpu
from jax.sharding import PartitionSpec as P

HALO = 4
LANES = 128
paganin_beta = 8.0
ramp_gain = 320.0


def split_np(x):
    high = x.astype(jnp.bfloat16)
    low = (x - high.astype(np.float64)).astype(jnp.bfloat16)
    return high, low


def split(x):
    high = x.astype(jnp.bfloat16)
    low = (x - high.astype(jnp.float32)).astype(jnp.bfloat16)
    return high, low


@functools.lru_cache(maxsize=None)
def tables(width, rows):
    blocks = width // LANES
    half = blocks // 2 + 1
    tile = rows + 2 * HALO
    lane = np.arange(LANES)
    t = np.arange(tile)
    basis, freq = [], []
    for u in range(tile // 2 + 1):
        scale = np.sqrt((1 if u in (0, tile / 2) else 2) / tile)
        basis.append(scale * np.cos(2 * np.pi * (u * t % tile) / tile))
        freq.append(u)
        if u not in (0, tile / 2):
            basis.append(scale * np.sin(2 * np.pi * (u * t % tile) / tile))
            freq.append(u)
    basis, freq = np.stack(basis), np.array(freq)
    own = basis[:, HALO : HALO + rows]
    top, bottom = basis[:, :HALO], basis[:, HALO + rows :]
    mix = []
    for first, second in ((bottom, top), (top, bottom)):
        high, low = split_np(np.concatenate([own, first, second], axis=1))
        mix.append(np.concatenate([high, high, low], axis=1))
    mix = np.stack(mix)
    high, low = split_np(own.T)
    back = np.concatenate([high, high, low], axis=1)
    k = np.arange(half)
    phase = 2 * np.pi * (k[:, None] * lane[None, :] % width) / width
    turn = np.stack([np.cos(phase), np.sin(phase)]).astype(np.float32)
    angle = 2 * np.pi * (lane[:, None] * lane[None, :] % LANES) / LANES
    c, s = np.cos(angle), np.sin(angle)
    forward = split_np(np.block([[c, -s], [s, c]]))
    inverse = split_np(np.block([[c, s], [-s, c]]))
    v = (k[:, None] + blocks * lane[None, :]).astype(np.float64)
    folded = np.minimum(v, width - v)
    ramp = ramp_gain * (folded / width) * (0.5 + 0.5 * np.cos(2 * np.pi * folded / width))
    weight = np.where((k == 0) | (2 * k == blocks), 1.0, 2.0)[:, None] / width
    lam = 4 * np.sin(np.pi * freq / tile)[None, :, None] ** 2 + 4 * np.sin(np.pi * v / width)[:, None, :] ** 2
    filt = ((ramp * weight)[:, None, :] / (1 + paganin_beta * lam)).astype(np.float32)
    column = LANES * np.arange(blocks + 1)[:, None, None] + lane[None, None, :]
    phase = 2 * np.pi * (k[None, :, None] * column % width) / width
    pad = -half % 8
    out_phase = np.stack([np.cos(phase), -np.sin(phase)], axis=1)
    out_phase = np.pad(out_phase, ((0, 0), (0, 0), (0, pad), (0, 0))).astype(np.float32)
    return mix, back, turn, *forward, *inverse, filt, out_phase


def real_dft(x):
    n = len(x)
    h = n // 2
    plus = {a: x[a] + x[n - a] for a in range(1, h)}
    minus = {a: x[a] - x[n - a] for a in range(1, h)}
    re, im = [None] * (h + 1), [None] * (h + 1)

    def total(terms):
        acc = None
        for c, y in terms:
            if abs(c) < 1e-12:
                continue
            z = y if c == 1.0 else (-y if c == -1.0 else y * np.float32(c))
            acc = z if acc is None else acc + z
        return acc

    def cos(m):
        return float(np.round(np.cos(2 * np.pi * (m % n) / n), 15))

    def sin(m):
        return float(np.round(np.sin(2 * np.pi * (m % n) / n), 15))

    for k in range(h // 2 + 1):
        ends = {0: x[0], h: x[h]}
        even = total([(cos(a * k), ends.get(a, plus.get(a))) for a in range(0, h + 1, 2)])
        odd = total([(cos(a * k), ends.get(a, plus.get(a))) for a in range(1, h + 1, 2)])
        re[k] = even if odd is None else even + odd
        re[h - k] = even if odd is None else even - odd
        even = total([(sin(a * k), minus[a]) for a in range(2, h, 2)])
        odd = total([(sin(a * k), minus[a]) for a in range(1, h, 2)])
        parts = [y for y in (even, odd) if y is not None]
        if parts:
            im[k] = -parts[0] if len(parts) == 1 else -(even + odd)
            if h - k != k:
                im[h - k] = (even - odd) if len(parts) == 2 else (even if odd is None else -odd)
    return re, im


def chain(regions, packed, starts, own, first, second, mix, back, turn, fwd_hi, fwd_lo, inv_hi, inv_lo, filt, out_phase, *rest):
    outs, (zhi, zlo, area) = rest[:-3], rest[-3:]
    rows, width = own.shape
    blocks = width // LANES
    half = blocks // 2 + 1
    tile = rows + 2 * HALO
    dot = functools.partial(jnp.dot, preferred_element_type=jnp.float32)
    parity = lax.rem(lax.axis_index("row"), 2)
    me = lax.axis_index("ang")
    halo = jnp.concatenate([first[...].astype(jnp.float32), second[...].astype(jnp.float32)], axis=0)
    high, low = split(jnp.concatenate([own[...], halo], axis=0))
    mixed = dot(mix[parity], jnp.concatenate([high, low, high], axis=0))
    pieces = []
    for j in range(0, tile, 8):
        pieces.append(real_dft([mixed[j : j + 8, LANES * a : LANES * (a + 1)] for a in range(blocks)]))
    for k in range(half):
        re = jnp.concatenate([p[0][k] for p in pieces], axis=0)
        c, s = turn[0, k : k + 1, :], turn[1, k : k + 1, :]
        if pieces[0][1][k] is None:
            turned = jnp.concatenate([re * c, -re * s], axis=1)
        else:
            im = jnp.concatenate([p[1][k] for p in pieces], axis=0)
            turned = jnp.concatenate([re * c + im * s, im * c - re * s], axis=1)
        zhi[k * tile : (k + 1) * tile, :], zlo[k * tile : (k + 1) * tile, :] = split(turned)
    spec = dot(zhi[...], fwd_hi[...]) + dot(zlo[...], fwd_hi[...]) + dot(zhi[...], fwd_lo[...])
    for k in range(half):
        part = spec[k * tile : (k + 1) * tile]
        g = filt[k]
        zhi[k * tile : (k + 1) * tile, :], zlo[k * tile : (k + 1) * tile, :] = split(
            jnp.concatenate([part[:, :LANES] * g, part[:, LANES:] * g], axis=1)
        )
    area[...] = dot(zhi[...], inv_hi[...]) + dot(zlo[...], inv_hi[...]) + dot(zhi[...], inv_lo[...])
    lanes = lax.broadcasted_iota(jnp.int32, (1, LANES), 1)

    def region(r):
        start = starts[me, r]
        block, offset = start // LANES, lax.rem(start, LANES)
        here, after = out_phase[block], out_phase[block + 1]
        phase = jnp.where((lanes >= offset)[None], here, after)
        acc = None
        for k in range(half):
            v = area[k * tile : (k + 1) * tile, :]
            term = v[:, :LANES] * phase[0, k : k + 1, :] + v[:, LANES:] * phase[1, k : k + 1, :]
            acc = term if acc is None else acc + term
        high, low = split(acc)
        value = dot(back[...], jnp.concatenate([high, low, high], axis=0))
        return value, offset

    if packed:
        cb = packed
        for i, out in enumerate(outs):
            value, offset = region(partner(me, i, regions))
            value = pltpu.roll(value, lax.rem(me * cb + LANES - offset, LANES), 1)
            keep = (lanes >= me * cb) & (lanes < (me + 1) * cb)
            out[...] = jnp.where(keep, value, 0.0).astype(out.dtype)
    else:

        @pl.loop(0, regions)
        def _(r):
            value, offset = region(r)
            outs[0][r] = pltpu.roll(value, lax.rem(LANES - offset, LANES), 1).astype(outs[0].dtype)


def partner(me, i, count):
    return me ^ i if count & (count - 1) == 0 else lax.rem(me + i, count)


def matchings(count):
    for begin in (0, 1):
        ends = [(i, i + 1) for i in range(begin, count - 1, 2)]
        yield ends + [(j, i) for i, j in ends]


def body(projections, flats, block_start, bp_weights):
    angles_dev, rows, width = projections.shape
    cb, pixels = bp_weights.shape[1:]
    regions, row_count = lax.axis_size("ang"), lax.axis_size("row")
    contrast = 1.0 - projections[0].astype(jnp.float32) / flats
    narrow = contrast.astype(jnp.bfloat16)
    initial, last = narrow[:HALO], narrow[rows - HALO :]
    even = lax.rem(lax.axis_index("row"), 2) == 0
    sent = (jnp.where(even, last, initial), jnp.where(even, initial, last))
    halo = [lax.ppermute(x, "row", pairs) if pairs else jnp.zeros_like(x) for x, pairs in zip(sent, matchings(row_count))]
    consts = tables(width, rows)
    packed = cb if regions * cb <= LANES else 0
    tile, half = rows + 2 * HALO, width // LANES // 2 + 1
    if packed:
        shapes = [jax.ShapeDtypeStruct((rows, LANES), jnp.bfloat16)] * regions
    else:
        shapes = [jax.ShapeDtypeStruct((regions, rows, LANES), jnp.bfloat16)]
    vmem = pl.BlockSpec(memory_space=pltpu.VMEM)
    blocks = pl.pallas_call(
        functools.partial(chain, regions, packed),
        out_shape=shapes,
        in_specs=[pl.BlockSpec(memory_space=pltpu.SMEM)] + [vmem] * (3 + len(consts)),
        out_specs=[vmem] * len(shapes),
        scratch_shapes=[
            pltpu.VMEM((half * tile, 2 * LANES), jnp.bfloat16),
            pltpu.VMEM((half * tile, 2 * LANES), jnp.bfloat16),
            pltpu.VMEM((half * tile, 2 * LANES), jnp.float32),
        ],
        name="chain",
    )(block_start, contrast, *halo, *map(jnp.asarray, consts))
    if packed:
        total = blocks[0]
        for i in range(1, regions):
            pairs = [(a, int(partner(a, i, regions))) if regions & (regions - 1) == 0 else (a, (a + i) % regions) for a in range(regions)]
            total = total + lax.ppermute(blocks[i], "ang", pairs)
        weights = bp_weights.reshape(regions * cb, pixels)
        return jnp.dot(total[:, : regions * cb], weights, preferred_element_type=jnp.float32)
    mine = lax.all_to_all(blocks[0][:, :, :cb], "ang", 0, 0, tiled=True)
    return jnp.einsum("arc,acp->rp", mine, bp_weights, preferred_element_type=jnp.float32)


def solution(mesh):
    placed = (P(("scan", "ang"), "row", None), P(("scan", "row"), None), P(), P(None, None, "ang"))
    return jax.shard_map(
        body, mesh=mesh, in_specs=placed, out_specs=P(("scan", "row"), "ang"), check_vma=False
    )
```

```python
import functools

import jax
import jax.numpy as jnp
import numpy as np
from jax import lax
from jax.experimental import pallas as pl
from jax.experimental.pallas import tpu as pltpu
from jax.sharding import PartitionSpec as P

HALO = 4
LANES = 128
paganin_beta = 8.0
ramp_gain = 320.0


def split_np(x):
    high = x.astype(jnp.bfloat16)
    low = (x - high.astype(np.float64)).astype(jnp.bfloat16)
    return high, low


def split(x):
    high = x.astype(jnp.bfloat16)
    low = (x - high.astype(jnp.float32)).astype(jnp.bfloat16)
    return high, low


@functools.lru_cache(maxsize=None)
def tables(width, rows):
    blocks = width // LANES
    half = blocks // 2 + 1
    depth = half + -half % 8
    tile = rows + 2 * HALO
    lane = np.arange(LANES)
    t = np.arange(tile)
    basis, freq = [], []
    for u in range(tile // 2 + 1):
        scale = np.sqrt((1 if u in (0, tile / 2) else 2) / tile)
        basis.append(scale * np.cos(2 * np.pi * (u * t % tile) / tile))
        freq.append(u)
        if u not in (0, tile / 2):
            basis.append(scale * np.sin(2 * np.pi * (u * t % tile) / tile))
            freq.append(u)
    basis, freq = np.stack(basis), np.array(freq)
    own = basis[:, HALO : HALO + rows]
    top, bottom = basis[:, :HALO], basis[:, HALO + rows :]
    high, low = split_np(own)
    mix = [np.concatenate([high, high, low], axis=1)]
    for first, second in ((bottom, top), (top, bottom)):
        mix.append(np.concatenate(split_np(np.concatenate([first, second], axis=1)), axis=1))
    high, low = split_np(own.T)
    back = np.concatenate([high, high, low], axis=1)
    k = np.arange(half)
    phase = 2 * np.pi * (k[:, None] * lane[None, :] % width) / width
    turn = [np.pad(x, ((0, depth - half), (0, 0))) for x in (np.cos(phase), np.sin(phase))]
    angle = 2 * np.pi * (lane[:, None] * lane[None, :] % LANES) / LANES
    c, s = np.cos(angle), np.sin(angle)
    forward = split_np(np.block([[c, -s], [s, c]]))
    v = (k[:, None] + blocks * lane[None, :]).astype(np.float64)
    folded = np.minimum(v, width - v)
    ramp = ramp_gain * (folded / width) * (0.5 + 0.5 * np.cos(2 * np.pi * folded / width))
    weight = np.where((k == 0) | (2 * k == blocks), 1.0, 2.0)[:, None] / width
    across = 4 * np.sin(np.pi * v / width) ** 2
    along = 4 * np.sin(np.pi * freq / tile)[:, None] ** 2
    parts = [np.pad(x, ((0, depth - half), (0, 0))) for x in (ramp * weight, 1 + paganin_beta * across)]
    parts += [np.broadcast_to(paganin_beta * along, (tile, LANES))]
    phase = 2 * np.pi * (k[:, None] * lane[None, :] % blocks) / blocks
    jump = [np.pad(x, ((0, depth - half), (0, 0))) for x in (np.cos(phase), np.sin(phase))]
    paired = np.concatenate(split_np(np.concatenate([*turn, *jump, *parts])), axis=1)
    parts = [*forward, paired, *mix, back]
    return np.concatenate([np.pad(x, ((0, -x.shape[0] % 16), (0, 2 * LANES - x.shape[1]))) for x in parts])


def layout(width, rows):
    blocks, half, depth, tile = sizes(width, rows)
    turn = 4 * LANES
    gain = turn + 4 * depth
    mix = gain + 2 * depth + tile
    return dict(turn=turn, jump=turn + 2 * depth, gain=gain, mix=mix, back=mix + 3 * tile)


def wide(table, begin, count):
    x = table[begin : begin + count, :].astype(jnp.float32)
    return x[:, :LANES] + x[:, LANES:]


def real_dft(x):
    n = len(x)
    h = n // 2
    plus = {a: x[a] + x[n - a] for a in range(1, h)}
    minus = {a: x[a] - x[n - a] for a in range(1, h)}
    re, im = [None] * (h + 1), [None] * (h + 1)

    def total(terms):
        acc = None
        for c, y in terms:
            if abs(c) < 1e-12:
                continue
            z = y if c == 1.0 else (-y if c == -1.0 else y * np.float32(c))
            acc = z if acc is None else acc + z
        return acc

    def cos(m):
        return float(np.round(np.cos(2 * np.pi * (m % n) / n), 15))

    def sin(m):
        return float(np.round(np.sin(2 * np.pi * (m % n) / n), 15))

    for k in range(h // 2 + 1):
        ends = {0: x[0], h: x[h]}
        even = total([(cos(a * k), ends.get(a, plus.get(a))) for a in range(0, h + 1, 2)])
        odd = total([(cos(a * k), ends.get(a, plus.get(a))) for a in range(1, h + 1, 2)])
        re[k] = even if odd is None else even + odd
        re[h - k] = even if odd is None else even - odd
        even = total([(sin(a * k), minus[a]) for a in range(2, h, 2)])
        odd = total([(sin(a * k), minus[a]) for a in range(1, h, 2)])
        parts = [y for y in (even, odd) if y is not None]
        if parts:
            im[k] = -parts[0] if len(parts) == 1 else -(even + odd)
            if h - k != k:
                im[h - k] = (even - odd) if len(parts) == 2 else (even if odd is None else -odd)
    return re, im


def sizes(width, rows):
    blocks = width // LANES
    half = blocks // 2 + 1
    return blocks, half, half + -half % 8, rows + 2 * HALO


dot = functools.partial(jnp.dot, preferred_element_type=jnp.float32)


def spectrum(mixed, table, zhi, zlo):
    tile, width = mixed.shape
    blocks, half, depth, _ = sizes(width, tile - 2 * HALO)
    turn = wide(table, layout(width, tile - 2 * HALO)["turn"], 2 * depth)
    pieces = []
    for j in range(0, tile, 8):
        pieces.append(real_dft([mixed[j : j + 8, LANES * a : LANES * (a + 1)] for a in range(blocks)]))
    for k in range(half):
        re = jnp.concatenate([p[0][k] for p in pieces], axis=0)
        c, s = turn[k : k + 1], turn[depth + k : depth + k + 1]
        if pieces[0][1][k] is None:
            turned = jnp.concatenate([re * c, -re * s], axis=1)
        else:
            im = jnp.concatenate([p[1][k] for p in pieces], axis=0)
            turned = jnp.concatenate([re * c + im * s, im * c - re * s], axis=1)
        zhi[k * tile : (k + 1) * tile, :], zlo[k * tile : (k + 1) * tile, :] = split(turned)
    n = 2 * LANES
    high, low = table[:n, :], table[n : 2 * n, :]
    return dot(zhi[...], high) + dot(zlo[...], high) + dot(zhi[...], low)


def prepare(regions, cb, starts, own, table, spec, filt, phases, shifts, zhi, zlo):
    rows, width = own.shape
    blocks, half, depth, tile = sizes(width, rows)
    at = layout(width, rows)
    me = lax.axis_index("ang")
    high, low = split(own[...])
    mix = table[at["mix"] : at["mix"] + tile, : 3 * rows]
    spec[...] = spectrum(dot(mix, jnp.concatenate([high, low, high], axis=0)), table, zhi, zlo)
    gain = wide(table, at["gain"], 2 * depth + tile)
    for k in range(half):
        lam = gain[2 * depth :] + gain[depth + k : depth + k + 1]
        filt[k * tile : (k + 1) * tile, :] = gain[k : k + 1] / lam
    lanes = lax.broadcasted_iota(jnp.int32, (1, LANES), 1)
    shifts[...] = jnp.zeros_like(shifts)
    turn, jump = wide(table, at["turn"], 2 * depth), wide(table, at["jump"], 2 * depth)

    def region(i):
        start = starts[me, partner(me, i, regions) if cb else i]
        block, offset = start // LANES, lax.rem(start, LANES)
        shifts[...] += jnp.where(lanes == i, lax.rem(me * cb + LANES - offset, LANES), 0).astype(jnp.float32)
        picked = []
        for b in (block, block + 1):
            picked.append(jnp.sum(jnp.where(lanes == b, jump, 0.0), axis=1, keepdims=True))
        far = jnp.where(lanes >= offset, picked[0], picked[1])
        c, s, fc, fs = turn[:depth], turn[depth:], far[:depth], far[depth:]
        phases[i] = jnp.concatenate([c * fc - s * fs, -(s * fc + c * fs)], axis=0)

    if cb:
        for i in range(regions):
            region(i)
    else:
        pl.loop(0, regions)(region)


def chain(regions, cb, first, second, table, spec, filt, phases, shifts, *rest):
    outs, (zhi, zlo, area) = rest[:-3], rest[-3:]
    width, rows = first.shape[1], outs[0].shape[-2]
    blocks, half, depth, tile = sizes(width, rows)
    where = layout(width, rows)
    n = 2 * LANES
    parity = lax.rem(lax.axis_index("row"), 2)
    halo = jnp.concatenate([first[...].astype(jnp.float32), second[...].astype(jnp.float32)], axis=0)
    halo = jnp.concatenate([halo, halo], axis=0).astype(jnp.bfloat16)
    mix = table[pl.ds(where["mix"] + pl.multiple_of((1 + parity) * tile, tile), tile), : 4 * HALO]
    whole = spectrum(dot(mix, halo), table, zhi, zlo)
    for k in range(half):
        at = slice(k * tile, (k + 1) * tile)
        part = whole[at] + spec[at, :]
        g = filt[at, :]
        zhi[at, :], zlo[at, :] = split(jnp.concatenate([part[:, :LANES] * g, part[:, LANES:] * g], axis=1))
    turned = functools.partial(lax.dot_general, dimension_numbers=(((1,), (1,)), ((), ())), preferred_element_type=jnp.float32)
    high, low = table[:n, :], table[n : 2 * n, :]
    area[...] = turned(zhi[...], high) + turned(zlo[...], high) + turned(zhi[...], low)
    lanes = lax.broadcasted_iota(jnp.int32, (1, LANES), 1)
    back = table[where["back"] : where["back"] + rows, : 3 * tile]

    def region(i):
        phase = phases[i]
        acc = None
        for k in range(half):
            v = area[k * tile : (k + 1) * tile, :]
            term = v[:, :LANES] * phase[k : k + 1] + v[:, LANES:] * phase[depth + k : depth + k + 1]
            acc = term if acc is None else acc + term
        high, low = split(acc)
        value = dot(back, jnp.concatenate([high, low, high], axis=0))
        return pltpu.roll(value, jnp.sum(jnp.where(lanes == i, shifts[...], 0.0)).astype(jnp.int32), 1)

    if cb:
        me = lax.axis_index("ang")
        keep = (lanes >= me * cb) & (lanes < (me + 1) * cb)
        for i, out in enumerate(outs):
            out[...] = jnp.where(keep, region(i), 0.0).astype(out.dtype)
    else:

        @pl.loop(0, regions)
        def _(r):
            outs[0][r] = region(r).astype(outs[0].dtype)


def partner(me, i, count):
    return me ^ i if count & (count - 1) == 0 else lax.rem(me + i, count)


def matchings(count):
    for begin in (0, 1):
        ends = [(i, i + 1) for i in range(begin, count - 1, 2)]
        yield ends + [(j, i) for i, j in ends]


def body(projections, flats, block_start, bp_weights):
    angles_dev, rows, width = projections.shape
    cb, pixels = bp_weights.shape[1:]
    regions, row_count = lax.axis_size("ang"), lax.axis_size("row")
    contrast = 1.0 - projections[0].astype(jnp.float32) / flats
    narrow = contrast.astype(jnp.bfloat16)
    initial, last = narrow[:HALO], narrow[rows - HALO :]
    even = lax.rem(lax.axis_index("row"), 2) == 0
    sent = (jnp.where(even, last, initial), jnp.where(even, initial, last))
    halo = []
    for name, x, pairs in zip(("hop_a", "hop_b"), sent, matchings(row_count)):
        with jax.named_scope(name):
            halo.append(lax.ppermute(x, "row", pairs) if pairs else jnp.zeros_like(x))
    table = jnp.asarray(tables(width, rows))
    packed = cb if regions * cb <= LANES else 0
    blocks, half, depth, tile = sizes(width, rows)
    vmem = pl.BlockSpec(memory_space=pltpu.VMEM)
    halves = [pltpu.VMEM((half * tile, 2 * LANES), jnp.bfloat16)] * 2
    limit = pltpu.CompilerParams(vmem_limit_bytes=8 * 1024 * 1024)
    ready = pl.pallas_call(
        functools.partial(prepare, regions, packed),
        out_shape=[
            jax.ShapeDtypeStruct((half * tile, 2 * LANES), jnp.float32),
            jax.ShapeDtypeStruct((half * tile, LANES), jnp.float32),
            jax.ShapeDtypeStruct((regions, 2 * depth, LANES), jnp.float32),
            jax.ShapeDtypeStruct((1, LANES), jnp.float32),
        ],
        in_specs=[pl.BlockSpec(memory_space=pltpu.SMEM), vmem, vmem],
        out_specs=[vmem] * 4,
        scratch_shapes=halves,
        compiler_params=limit,
        cost_estimate=pl.CostEstimate(flops=400_000_000, bytes_accessed=2_000_000, transcendentals=0),
        name="prepare",
    )(block_start, contrast, table)
    if packed:
        shapes = [jax.ShapeDtypeStruct((rows, LANES), jnp.bfloat16)] * regions
    else:
        shapes = [jax.ShapeDtypeStruct((regions, rows, LANES), jnp.bfloat16)]
    cut = pl.pallas_call(
        functools.partial(chain, regions, packed),
        out_shape=shapes,
        in_specs=[vmem] * 7,
        out_specs=[vmem] * len(shapes),
        scratch_shapes=halves + [pltpu.VMEM((half * tile, 2 * LANES), jnp.float32)],
        compiler_params=limit,
        name="chain",
    )(*halo, table, *ready)
    if packed:
        total = cut[0]
        for i in reversed(range(1, regions)):
            pairs = [(a, int(partner(a, i, regions)) if regions & (regions - 1) == 0 else (a + i) % regions) for a in range(regions)]
            with jax.named_scope(f"ang_{i}"):
                total = total + lax.ppermute(cut[i], "ang", pairs)
        weights = bp_weights.reshape(regions * cb, pixels)
        return jnp.dot(total[:, : regions * cb], weights, preferred_element_type=jnp.float32)
    mine = lax.all_to_all(cut[0][:, :, :cb], "ang", 0, 0, tiled=True)
    return jnp.einsum("arc,acp->rp", mine, bp_weights, preferred_element_type=jnp.float32)


def solution(mesh):
    placed = (P(("scan", "ang"), "row", None), P(("scan", "row"), None), P(), P(None, None, "ang"))
    return jax.shard_map(
        body, mesh=mesh, in_specs=placed, out_specs=P(("scan", "row"), "ang"), check_vma=False
    )
```

```python
import functools

import jax
import jax.numpy as jnp
import numpy as np
from jax import lax
from jax.experimental import pallas as pl
from jax.experimental.pallas import tpu as pltpu
from jax.sharding import PartitionSpec as P


HALO = 4
LANES = 128
RING = (0, 2, 1, 3)
paganin_beta = 8.0
ramp_gain = 320.0


def split(x):
    high = x.astype(jnp.bfloat16)
    low = (x - high.astype(jnp.float32)).astype(jnp.bfloat16)
    return high, low


def sizes(width, rows):
    blocks = width // LANES
    half = blocks // 2 + 1
    return blocks, half, half + -half % 8, rows + 2 * HALO


def wave(j, period):
    y = (2 * j - period).astype(jnp.float32) * np.float32(np.pi / (2 * period))
    z = y * y
    p = np.float32(-1 / 39916800)
    for c in (1 / 362880, -1 / 5040, 1 / 120, -1 / 6, 1.0):
        p = p * z + np.float32(c)
    y = y * p
    return 2.0 * y * y - 1.0


def late(j, period):
    return jnp.where(j >= period // 4, j - period // 4, j + period - period // 4)


def iotas(rows, lanes=LANES):
    return (lax.broadcasted_iota(jnp.int32, (rows, lanes), d) for d in (0, 1))


def matrices(m_high, m_low):
    row, col = iotas(LANES)
    c, s = wave(row * col & (LANES - 1), LANES), wave((row * col - LANES // 4) & (LANES - 1), LANES)
    for ref, c, s in zip((m_high, m_low), split(c), split(s)):
        ref[:LANES, :LANES], ref[:LANES, LANES:] = c, -s
        ref[LANES:, :LANES], ref[LANES:, LANES:] = s, c


def real_dft(x):
    n = len(x)
    h = n // 2
    plus = {a: x[a] + x[n - a] for a in range(1, h)}
    minus = {a: x[a] - x[n - a] for a in range(1, h)}
    re, im = [None] * (h + 1), [None] * (h + 1)

    def total(terms):
        acc = None
        for c, y in terms:
            if abs(c) < 1e-12:
                continue
            z = y if c == 1.0 else (-y if c == -1.0 else y * np.float32(c))
            acc = z if acc is None else acc + z
        return acc

    def cos(m):
        return float(np.round(np.cos(2 * np.pi * (m % n) / n), 15))

    def sin(m):
        return float(np.round(np.sin(2 * np.pi * (m % n) / n), 15))

    for k in range(h // 2 + 1):
        ends = {0: x[0], h: x[h]}
        even = total([(cos(a * k), ends.get(a, plus.get(a))) for a in range(0, h + 1, 2)])
        odd = total([(cos(a * k), ends.get(a, plus.get(a))) for a in range(1, h + 1, 2)])
        re[k] = even if odd is None else even + odd
        re[h - k] = even if odd is None else even - odd
        even = total([(sin(a * k), minus[a]) for a in range(2, h, 2)])
        odd = total([(sin(a * k), minus[a]) for a in range(1, h, 2)])
        parts = [y for y in (even, odd) if y is not None]
        if parts:
            im[k] = -parts[0] if len(parts) == 1 else -(even + odd)
            if h - k != k:
                im[h - k] = (even - odd) if len(parts) == 2 else (even if odd is None else -odd)
    return re, im


def product(passes, high, low, x, m_high, m_low, turned):
    dims = (((1,), (1 if turned else 0,)), ((), ()))
    dot = functools.partial(lax.dot_general, dimension_numbers=dims, preferred_element_type=jnp.float32)
    n = x[0].shape[0]
    for k, part in enumerate(x):
        at = slice(k * n, (k + 1) * n)
        if passes == 1:
            high[at, :] = part.astype(jnp.bfloat16)
        else:
            high[at, :], low[at, :] = split(part)
    out = dot(high[...], m_high)
    if passes > 1:
        out += dot(low[...], m_high)
    if passes > 2:
        out += dot(high[...], m_low)
    return out


def filtered(passes, x, begins, m_high, m_low, kern, turn, high, low, spec):
    rows, blocks = x[0].shape[0], len(x)
    _, half, depth, _ = sizes(blocks * LANES, rows)
    m_high, m_low = m_high[...], m_low[...] if passes > 2 else None
    re, im = real_dft(x)
    parts = []
    for k in range(half):
        c, s = turn[k : k + 1], turn[depth + k : depth + k + 1]
        if im[k] is None:
            parts.append(jnp.concatenate([re[k] * c, -re[k] * s], axis=1))
        else:
            parts.append(jnp.concatenate([re[k] * c + im[k] * s, im[k] * c - re[k] * s], axis=1))
    spec[...] = product(passes, high, low, parts, m_high, m_low, False)
    parts = []
    for k in range(half):
        re = im = None
        for t, begin in enumerate(begins):
            entry = kern[k, pl.ds(begin, rows), :]
            row = k * rows + t
            a, b = entry * spec[row : row + 1, :LANES], entry * spec[row : row + 1, LANES:]
            re, im = (a, b) if re is None else (re + a, im + b)
        parts.append(jnp.concatenate([re, im], axis=1))
    return product(passes, high, low, parts, m_high, m_low, True)


def begin(proj_in, flats_in, starts_in, own, first, second, starts, proj, flats, sems):
    rows, width = own.shape
    pieces = sems.shape[0] // 2
    step = width // pieces
    late = pltpu.make_async_copy(starts_in, starts, sems.at[2 * pieces])
    copies = []
    for i in range(pieces):
        at = pl.ds(i * step, step)
        copies.append(pltpu.make_async_copy(flats_in.at[:, at], flats.at[:, at], sems.at[2 * i]))
        copies.append(pltpu.make_async_copy(proj_in.at[0, :, at], proj.at[:, at], sems.at[2 * i + 1]))
    for copy in (*copies, late):
        copy.start()
    even = lax.rem(lax.axis_index("row"), 2) == 0
    for i in range(pieces):
        copies[2 * i].wait()
        copies[2 * i + 1].wait()
        at = slice(i * step, (i + 1) * step)
        contrast = 1.0 - proj[:, at].astype(jnp.float32) / flats[:, at]
        own[:, at] = contrast
        initial, last = contrast[:HALO], contrast[rows - HALO :]
        first[:, at] = jnp.where(even, last, initial).astype(first.dtype)
        second[:, at] = jnp.where(even, initial, last).astype(second.dtype)
    late.wait()


def each(count, packed, f):
    if packed:
        for i in range(count):
            f(i)
    else:
        pl.loop(0, count)(f)


def prepare(own, m_high, kern, back, turn, jump, high, low, spec, m_low):
    rows, width = own.shape
    blocks, half, depth, tile = sizes(width, rows)
    spread = rows + HALO
    matrices(m_high, m_low)
    k, lane = iotas(depth)
    turn[:depth, :], turn[depth:, :] = wave(k * lane, width), wave(late(k * lane, width), width)
    around = lax.rem(k * lane, blocks)
    jump[:depth, :], jump[depth:, :] = wave(around, blocks), wave(lax.rem(around + blocks - blocks // 4, blocks), blocks)
    v = k + blocks * lane
    folded = jnp.minimum(v, width - v)
    part = jnp.where((k == 0) | (2 * k == blocks), 1.0 / width, 2.0 / width)
    folded_wave = wave(folded, width)
    gain = ramp_gain * (folded.astype(jnp.float32) / width) * (0.5 + 0.5 * folded_wave) * part
    across = 1.0 + paganin_beta * (2.0 - 2.0 * folded_wave)
    u, _ = iotas(tile)
    along = paganin_beta * (2.0 - 2.0 * wave(u, tile))
    parts = [gain[k : k + 1] / (along + across[k : k + 1]) for k in range(half)]
    f_high, f_low = split(jnp.concatenate(parts, axis=1))
    i, u = iotas(2 * spread, tile)
    count = jnp.where(2 * u > tile, 0.0, jnp.where((u == 0) | (2 * u == tile), 1.0 / tile, 2.0 / tile))
    mix_high, mix_low = split(count * wave(lax.rem((i + tile * spread - spread) * u, tile), tile))
    dot = functools.partial(jnp.dot, preferred_element_type=jnp.float32)
    entries = dot(mix_high, f_high) + dot(mix_high, f_low) + dot(mix_low, f_high)
    for k in range(half):
        kern[k] = entries[:, k * LANES : (k + 1) * LANES]
    x = [own[:, LANES * a : LANES * (a + 1)] for a in range(blocks)]
    back[...] = filtered(3, x, [spread - t for t in range(rows)], m_high, m_low, kern, turn, high, low, spec)


def chain(regions, packed, first, second, starts, m_high, kern, own_back, turn, jump, *rest):
    outs, (high, low, spec, back) = rest[:-4], rest[-4:]
    width, rows = first.shape[1], kern.shape[1] // 2 - HALO
    blocks, half, depth, _ = sizes(width, rows)
    spread = rows + HALO
    row, me = lax.axis_index("row"), lax.axis_index("ang")
    even = lax.rem(row, 2) == 0
    got, other = first[...].astype(jnp.float32), second[...].astype(jnp.float32)
    above = jnp.where(row == 0, 0.0, jnp.where(even, other, got))
    below = jnp.where(row == lax.axis_size("row") - 1, 0.0, jnp.where(even, got, other))
    x = jnp.concatenate([above, below], axis=0)
    begins = [spread + HALO - t for t in range(HALO)] + [spread - rows - t for t in range(HALO)]
    x = [x[:, LANES * a : LANES * (a + 1)] for a in range(blocks)]
    back[...] = filtered(PASSES, x, begins, m_high, None, kern, turn, high, low, spec) + own_back[...]
    lanes = lax.broadcasted_iota(jnp.int32, (1, LANES), 1).astype(jnp.float32)
    angle, column = iotas(*starts.shape)
    mine = jnp.where(angle == me, starts[...].astype(jnp.float32), 0.0)
    c, s = turn[:depth, :], turn[depth:, :]

    def region(i):
        start = jnp.where(column == (target(me, i, regions) if packed else i), mine, 0.0)
        start = jnp.sum(jnp.sum(start, axis=1, keepdims=True), axis=0, keepdims=True)
        block = jnp.floor(start * (1.0 / LANES))
        near, far = (jnp.sum(jnp.where(lanes == b, jump[...], 0.0), axis=1, keepdims=True) for b in (block, block + 1.0))
        far = jnp.where(lanes >= start - LANES * block, near, far)
        fc, fs = far[:depth], far[depth:]
        phase = jnp.concatenate([c * fc - s * fs, -(s * fc + c * fs)], axis=0)
        value = None
        for k in range(half):
            v = back[k * rows : (k + 1) * rows, :]
            term = v[:, :LANES] * phase[k : k + 1] + v[:, LANES:] * phase[depth + k : depth + k + 1]
            value = term if value is None else value + term
        if packed:
            outs[i][...] = value.astype(jnp.bfloat16)
        else:
            outs[0][i] = value.astype(jnp.bfloat16)

    each(regions, packed, region)


PASSES = 1
PIECES = 2


def place(angles, packed, starts, weights, placed):
    cb = weights.shape[1]
    me = lax.axis_index("ang")

    def one(i):
        a = source(me, i, angles) if packed else i
        offset = lax.rem(starts[a, me], LANES)
        spot = lax.broadcasted_iota(jnp.int32, (LANES, cb), 0) - lax.broadcasted_iota(jnp.int32, (LANES, cb), 1)
        spot = ((spot == offset) | (spot == offset - LANES)).astype(jnp.float32).astype(jnp.bfloat16)
        value = jnp.dot(spot, weights[a], preferred_element_type=jnp.float32).astype(placed.dtype)
        placed[pl.ds(pl.multiple_of(i * LANES, LANES), LANES) if not packed else pl.ds(i * LANES, LANES), :] = value

    each(angles, packed, one)


def finish(blocks, packed, *refs):
    *cut, placed, out = refs
    dot = functools.partial(jnp.dot, preferred_element_type=jnp.float32)
    if packed:
        out[...] = dot(jnp.concatenate([x[...] for x in cut], axis=1), placed[...])
    else:
        out[...] = jnp.zeros_like(out)

        @pl.loop(0, blocks)
        def _(a):
            out[...] += dot(cut[0][a], placed[pl.ds(pl.multiple_of(a * LANES, LANES), LANES), :])


def rounds(count):
    ring = RING if count == len(RING) else range(count)
    place = {x: p for p, x in enumerate(ring)}
    return [[ring[(place[x] + i) % count] for x in range(count)] for i in range(count)]


def pick(me, values):
    out = jnp.int32(0)
    for x, y in enumerate(values):
        out = jnp.where(me == x, y, out)
    return out


def target(me, i, count):
    return pick(me, rounds(count)[i])


def source(me, i, count):
    return pick(me, rounds(count)[-i % count])


def matchings(count):
    for start in (0, 1):
        ends = [(i, i + 1) for i in range(start, count - 1, 2)]
        if start and count % 2 == 0:
            ends.append((count - 1, 0))
        yield [pair for i, j in ends for pair in ((i, j), (j, i))]


def body(projections, flats, block_start, bp_weights):
    _, rows, width = projections.shape
    angles, _, pixels = bp_weights.shape
    regions, row_count = lax.axis_size("ang"), lax.axis_size("row")
    _, half, depth, _ = sizes(width, rows)
    f32, bf16 = jnp.float32, jnp.bfloat16
    shape = jax.ShapeDtypeStruct
    vmem = pl.BlockSpec(memory_space=pltpu.VMEM)
    limit = pltpu.CompilerParams(vmem_limit_bytes=12 * 1024 * 1024)
    packed = regions <= len(RING)
    pieces = PIECES if width % (PIECES * LANES) == 0 else 1
    hbm = pl.BlockSpec(memory_space=pltpu.HBM)
    contrast, *sent, starts = pl.pallas_call(
        begin,
        out_shape=[shape((rows, width), f32)] + [shape((HALO, width), bf16)] * 2 + [shape(block_start.shape, block_start.dtype)],
        in_specs=[hbm] * 3,
        out_specs=[vmem] * 4,
        scratch_shapes=[
            pltpu.VMEM((rows, width), bf16),
            pltpu.VMEM((rows, width), f32),
            pltpu.SemaphoreType.DMA((2 * pieces + 1,)),
        ],
        compiler_params=limit,
        name="begin",
    )(*(pltpu.with_memory_space_constraint(x, pltpu.HBM) for x in (projections, flats, block_start)))
    scratch = [pltpu.VMEM((half * rows, 2 * LANES), t) for t in (bf16, bf16, f32, f32)]
    work = pl.pallas_call(
        prepare,
        out_shape=[
            shape((2 * LANES, 2 * LANES), bf16),
            shape((half, 2 * (rows + HALO), LANES), f32),
            shape((half * rows, 2 * LANES), f32),
            shape((2 * depth, LANES), f32),
            shape((2 * depth, LANES), f32),
        ],
        in_specs=[vmem],
        out_specs=[vmem] * 5,
        scratch_shapes=scratch[:3] + [pltpu.VMEM((2 * LANES, 2 * LANES), bf16)],
        compiler_params=limit,
        cost_estimate=pl.CostEstimate(flops=400_000_000, bytes_accessed=2_000_000, transcendentals=0),
        name="prepare",
    )
    near, far = matchings(row_count)
    first = lax.ppermute(sent[0], "row", near)

    def edge(contrast, x):
        return x, *work(contrast)

    def inner(contrast, x):
        x = lax.ppermute(x, "row", far)
        return x, *work(contrast)

    row = lax.axis_index("row")
    second, m_high, *ready = lax.cond((row == 0) | (row == row_count - 1), edge, inner, contrast, sent[1])
    cut = pl.pallas_call(
        functools.partial(chain, regions, packed),
        out_shape=[shape((rows, LANES), bf16)] * regions if packed else [shape((regions, rows, LANES), bf16)],
        in_specs=[vmem] * 8,
        out_specs=[vmem] * (regions if packed else 1),
        scratch_shapes=scratch,
        compiler_params=limit,
        name="chain",
    )(first, second, starts, m_high, *ready)
    if packed:
        mine = [cut[0]]
        for i in range(1, regions):
            mine.append(lax.ppermute(cut[i], "ang", list(enumerate(rounds(regions)[i]))))
    else:
        mine = [lax.all_to_all(cut[0], "ang", 0, 0, tiled=True)]
    placed = pl.pallas_call(
        functools.partial(place, angles, packed),
        out_shape=shape((angles * LANES, pixels), bf16),
        in_specs=[pl.BlockSpec(memory_space=pltpu.SMEM), vmem],
        out_specs=vmem,
        compiler_params=limit,
        cost_estimate=pl.CostEstimate(flops=100_000_000, bytes_accessed=400_000, transcendentals=0),
        name="place",
    )(block_start, bp_weights)
    return pl.pallas_call(
        functools.partial(finish, angles, packed),
        out_shape=shape((rows, pixels), f32),
        in_specs=[vmem] * (len(mine) + 1),
        out_specs=vmem,
        compiler_params=limit,
        name="finish",
    )(*mine, placed)


def solution(mesh):
    placed = (P(("scan", "ang"), "row", None), P(("scan", "row"), None), P(), P(None, None, "ang"))
    return jax.shard_map(body, mesh=mesh, in_specs=placed, out_specs=P(("scan", "row"), "ang"), check_vma=False)
```

```python
import functools

import jax
import jax.numpy as jnp
import numpy as np
from jax import lax
from jax.experimental import pallas as pl
from jax.experimental.pallas import tpu as pltpu
from jax.sharding import PartitionSpec as P


HALO = 4
LANES = 128
RING = (0, 2, 1, 3)
paganin_beta = 8.0
ramp_gain = 320.0


def split(x):
    high = x.astype(jnp.bfloat16)
    low = (x - high.astype(jnp.float32)).astype(jnp.bfloat16)
    return high, low


def sizes(width, rows):
    blocks = width // LANES
    half = blocks // 2 + 1
    return blocks, half, half + -half % 8, rows + 2 * HALO


def wave(j, period):
    y = (2 * j - period).astype(jnp.float32) * np.float32(np.pi / (2 * period))
    z = y * y
    p = np.float32(-1 / 39916800)
    for c in (1 / 362880, -1 / 5040, 1 / 120, -1 / 6, 1.0):
        p = p * z + np.float32(c)
    y = y * p
    return 2.0 * y * y - 1.0


def late(j, period):
    return jnp.where(j >= period // 4, j - period // 4, j + period - period // 4)


def iotas(rows, lanes=LANES):
    return (lax.broadcasted_iota(jnp.int32, (rows, lanes), d) for d in (0, 1))


def matrices(m_high, m_low):
    row, col = iotas(LANES)
    c, s = wave(row * col & (LANES - 1), LANES), wave((row * col - LANES // 4) & (LANES - 1), LANES)
    for ref, c, s in zip((m_high, m_low), split(c), split(s)):
        ref[:LANES, :LANES], ref[:LANES, LANES:] = c, -s
        ref[LANES:, :LANES], ref[LANES:, LANES:] = s, c


def real_dft(x):
    n = len(x)
    h = n // 2
    plus = {a: x[a] + x[n - a] for a in range(1, h)}
    minus = {a: x[a] - x[n - a] for a in range(1, h)}
    re, im = [None] * (h + 1), [None] * (h + 1)

    def total(terms):
        acc = None
        for c, y in terms:
            if abs(c) < 1e-12:
                continue
            z = y if c == 1.0 else (-y if c == -1.0 else y * np.float32(c))
            acc = z if acc is None else acc + z
        return acc

    def cos(m):
        return float(np.round(np.cos(2 * np.pi * (m % n) / n), 15))

    def sin(m):
        return float(np.round(np.sin(2 * np.pi * (m % n) / n), 15))

    for k in range(h // 2 + 1):
        ends = {0: x[0], h: x[h]}
        even = total([(cos(a * k), ends.get(a, plus.get(a))) for a in range(0, h + 1, 2)])
        odd = total([(cos(a * k), ends.get(a, plus.get(a))) for a in range(1, h + 1, 2)])
        re[k] = even if odd is None else even + odd
        re[h - k] = even if odd is None else even - odd
        even = total([(sin(a * k), minus[a]) for a in range(2, h, 2)])
        odd = total([(sin(a * k), minus[a]) for a in range(1, h, 2)])
        parts = [y for y in (even, odd) if y is not None]
        if parts:
            im[k] = -parts[0] if len(parts) == 1 else -(even + odd)
            if h - k != k:
                im[h - k] = (even - odd) if len(parts) == 2 else (even if odd is None else -odd)
    return re, im


def product(passes, high, low, x, m_high, m_low, turned):
    dims = (((1,), (1 if turned else 0,)), ((), ()))
    dot = functools.partial(lax.dot_general, dimension_numbers=dims, preferred_element_type=jnp.float32)
    n = x[0].shape[0]
    for k, part in enumerate(x):
        at = slice(k * n, (k + 1) * n)
        if passes == 1:
            high[at, :] = part.astype(jnp.bfloat16)
        else:
            high[at, :], low[at, :] = split(part)
    out = dot(high[...], m_high)
    if passes > 1:
        out += dot(low[...], m_high)
    if passes > 2:
        out += dot(high[...], m_low)
    return out


def filtered(passes, x, begins, m_high, m_low, kern, turn, high, low, spec):
    rows, blocks = x[0].shape[0], len(x)
    _, half, depth, _ = sizes(blocks * LANES, rows)
    m_high, m_low = m_high[...], m_low[...] if passes > 2 else None
    re, im = real_dft(x)
    parts = []
    for k in range(half):
        c, s = turn[k : k + 1], turn[depth + k : depth + k + 1]
        if im[k] is None:
            parts.append(jnp.concatenate([re[k] * c, -re[k] * s], axis=1))
        else:
            parts.append(jnp.concatenate([re[k] * c + im[k] * s, im[k] * c - re[k] * s], axis=1))
    spec[...] = product(passes, high, low, parts, m_high, m_low, False)
    parts = []
    for k in range(half):
        re = im = None
        for t, begin in enumerate(begins):
            entry = kern[k, pl.ds(begin, rows), :]
            row = k * rows + t
            a, b = entry * spec[row : row + 1, :LANES], entry * spec[row : row + 1, LANES:]
            re, im = (a, b) if re is None else (re + a, im + b)
        parts.append(jnp.concatenate([re, im], axis=1))
    return product(passes, high, low, parts, m_high, m_low, True)


def begin(proj_in, flats_in, starts_in, own, first, second, starts, proj, flats, sems):
    rows, width = own.shape
    pieces = sems.shape[0] // 2
    step = width // pieces
    late = pltpu.make_async_copy(starts_in, starts, sems.at[2 * pieces])
    copies = []
    for i in range(pieces):
        at = pl.ds(i * step, step)
        copies.append(pltpu.make_async_copy(flats_in.at[:, at], flats.at[:, at], sems.at[2 * i]))
        copies.append(pltpu.make_async_copy(proj_in.at[0, :, at], proj.at[:, at], sems.at[2 * i + 1]))
    for copy in (*copies, late):
        copy.start()
    even = lax.rem(lax.axis_index("row"), 2) == 0
    for i in range(pieces):
        copies[2 * i].wait()
        copies[2 * i + 1].wait()
        at = slice(i * step, (i + 1) * step)
        contrast = 1.0 - proj[:, at].astype(jnp.float32) / flats[:, at]
        own[:, at] = contrast
        initial, last = contrast[:HALO], contrast[rows - HALO :]
        first[:, at] = jnp.where(even, last, initial).astype(first.dtype)
        second[:, at] = jnp.where(even, initial, last).astype(second.dtype)
    late.wait()


def each(count, packed, f):
    if packed:
        for i in range(count):
            f(i)
    else:
        pl.loop(0, count)(f)


def prepare(regions, packed, own, starts, m_high, near, back, phases, turn, kern, high, low, spec, m_low):
    rows, width = own.shape
    blocks, half, depth, tile = sizes(width, rows)
    spread = rows + HALO
    matrices(m_high, m_low)
    k, lane = iotas(depth)
    turn[:depth, :], turn[depth:, :] = wave(k * lane, width), wave(late(k * lane, width), width)
    around = lax.rem(k * lane, blocks)
    jump = jnp.concatenate([wave(around, blocks), wave(lax.rem(around + blocks - blocks // 4, blocks), blocks)], axis=0)
    v = k + blocks * lane
    folded = jnp.minimum(v, width - v)
    part = jnp.where((k == 0) | (2 * k == blocks), 1.0 / width, 2.0 / width)
    folded_wave = wave(folded, width)
    gain = ramp_gain * (folded.astype(jnp.float32) / width) * (0.5 + 0.5 * folded_wave) * part
    across = 1.0 + paganin_beta * (2.0 - 2.0 * folded_wave)
    u, _ = iotas(tile)
    along = paganin_beta * (2.0 - 2.0 * wave(u, tile))
    parts = [gain[k : k + 1] / (along + across[k : k + 1]) for k in range(half)]
    f_high, f_low = split(jnp.concatenate(parts, axis=1))
    i, u = iotas(2 * spread, tile)
    count = jnp.where(2 * u > tile, 0.0, jnp.where((u == 0) | (2 * u == tile), 1.0 / tile, 2.0 / tile))
    mix_high, mix_low = split(count * wave(lax.rem((i + tile * spread - spread) * u, tile), tile))
    dot = functools.partial(jnp.dot, preferred_element_type=jnp.float32)
    entries = dot(mix_high, f_high) + dot(mix_high, f_low) + dot(mix_low, f_high)
    row, me = lax.axis_index("row"), lax.axis_index("ang")
    even = lax.rem(row, 2) == 0
    inside = (row > 0) & (row < lax.axis_size("row") - 1)
    reach = rows + HALO - 1
    for k in range(half):
        kern[k] = entries[:, k * LANES : (k + 1) * LANES]
        below, above = kern[k, 1 : 1 + reach, :], kern[k, 2 * spread - reach : 2 * spread, :]
        near[k, :reach, :] = jnp.where(even, below, above)
        near[k, 2 * rows : 2 * rows + reach, :] = jnp.where(inside, jnp.where(even, above, below), 0.0)
    lanes = lax.broadcasted_iota(jnp.int32, (1, LANES), 1).astype(jnp.float32)
    angle, column = iotas(*starts.shape)
    mine = jnp.where(angle == me, starts[...].astype(jnp.float32), 0.0)
    c, s = turn[:depth, :], turn[depth:, :]

    def phase(i):
        start = jnp.where(column == (target(me, i, regions) if packed else i), mine, 0.0)
        start = jnp.sum(jnp.sum(start, axis=1, keepdims=True), axis=0, keepdims=True)
        block = jnp.floor(start * (1.0 / LANES))
        here, after = (jnp.sum(jnp.where(lanes == b, jump, 0.0), axis=1, keepdims=True) for b in (block, block + 1.0))
        far = jnp.where(lanes >= start - LANES * block, here, after)
        fc, fs = far[:depth], far[depth:]
        phases[i] = jnp.concatenate([c * fc - s * fs, -(s * fc + c * fs)], axis=0)

    each(regions, packed, phase)
    x = [own[:, LANES * a : LANES * (a + 1)] for a in range(blocks)]
    back[...] = filtered(3, x, [spread - t for t in range(rows)], m_high, m_low, kern, turn, high, low, spec)


def chain(regions, packed, first, second, m_high, near, own_back, phases, turn, *rest):
    outs, (high, low, spec, back) = rest[:-4], rest[-4:]
    width, rows = first.shape[1], near.shape[1] // 4
    blocks, half, depth, _ = sizes(width, rows)
    x = jnp.concatenate([first[...].astype(jnp.float32), second[...].astype(jnp.float32)], axis=0)
    begins = [begin + HALO - 1 - t for begin in (0, 2 * rows) for t in range(HALO)]
    x = [x[:, LANES * a : LANES * (a + 1)] for a in range(blocks)]
    back[...] = filtered(PASSES, x, begins, m_high, None, near, turn, high, low, spec) + own_back[...]

    def region(i):
        value = None
        for k in range(half):
            v = back[k * rows : (k + 1) * rows, :]
            term = v[:, :LANES] * phases[i, k : k + 1, :] + v[:, LANES:] * phases[i, depth + k : depth + k + 1, :]
            value = term if value is None else value + term
        if packed:
            outs[i][...] = value.astype(jnp.bfloat16)
        else:
            outs[0][i] = value.astype(jnp.bfloat16)

    each(regions, packed, region)


PASSES = 1
PIECES = 2


def place(angles, packed, starts, weights, placed):
    cb = weights.shape[1]
    me = lax.axis_index("ang")

    def one(i):
        a = source(me, i, angles) if packed else i
        offset = lax.rem(starts[a, me], LANES)
        spot = lax.broadcasted_iota(jnp.int32, (LANES, cb), 0) - lax.broadcasted_iota(jnp.int32, (LANES, cb), 1)
        spot = ((spot == offset) | (spot == offset - LANES)).astype(jnp.float32).astype(jnp.bfloat16)
        value = jnp.dot(spot, weights[a], preferred_element_type=jnp.float32).astype(placed.dtype)
        placed[pl.ds(pl.multiple_of(i * LANES, LANES), LANES) if not packed else pl.ds(i * LANES, LANES), :] = value

    each(angles, packed, one)


def finish(blocks, packed, *refs):
    *cut, placed, out = refs
    dot = functools.partial(jnp.dot, preferred_element_type=jnp.float32)
    if packed:
        out[...] = dot(jnp.concatenate([x[...] for x in cut], axis=1), placed[...])
    else:
        out[...] = jnp.zeros_like(out)

        @pl.loop(0, blocks)
        def _(a):
            out[...] += dot(cut[0][a], placed[pl.ds(pl.multiple_of(a * LANES, LANES), LANES), :])


def rounds(count):
    ring = RING if count == len(RING) else range(count)
    place = {x: p for p, x in enumerate(ring)}
    return [[ring[(place[x] + i) % count] for x in range(count)] for i in range(count)]


def pick(me, values):
    out = jnp.int32(0)
    for x, y in enumerate(values):
        out = jnp.where(me == x, y, out)
    return out


def target(me, i, count):
    return pick(me, rounds(count)[i])


def source(me, i, count):
    return pick(me, rounds(count)[-i % count])


def matchings(count):
    for start in (0, 1):
        ends = [(i, i + 1) for i in range(start, count - 1, 2)]
        if start and count % 2 == 0:
            ends.append((count - 1, 0))
        yield [pair for i, j in ends for pair in ((i, j), (j, i))]


def body(projections, flats, block_start, bp_weights):
    _, rows, width = projections.shape
    angles, _, pixels = bp_weights.shape
    regions, row_count = lax.axis_size("ang"), lax.axis_size("row")
    _, half, depth, _ = sizes(width, rows)
    f32, bf16 = jnp.float32, jnp.bfloat16
    shape = jax.ShapeDtypeStruct
    vmem = pl.BlockSpec(memory_space=pltpu.VMEM)
    limit = pltpu.CompilerParams(vmem_limit_bytes=12 * 1024 * 1024)
    packed = regions <= len(RING)
    pieces = PIECES if width % (PIECES * LANES) == 0 else 1
    hbm = pl.BlockSpec(memory_space=pltpu.HBM)
    contrast, *sent, starts = pl.pallas_call(
        begin,
        out_shape=[shape((rows, width), f32)] + [shape((HALO, width), bf16)] * 2 + [shape(block_start.shape, block_start.dtype)],
        in_specs=[hbm] * 3,
        out_specs=[vmem] * 4,
        scratch_shapes=[
            pltpu.VMEM((rows, width), bf16),
            pltpu.VMEM((rows, width), f32),
            pltpu.SemaphoreType.DMA((2 * pieces + 1,)),
        ],
        compiler_params=limit,
        name="begin",
    )(*(pltpu.with_memory_space_constraint(x, pltpu.HBM) for x in (projections, flats, block_start)))
    scratch = [pltpu.VMEM((half * rows, 2 * LANES), t) for t in (bf16, bf16, f32, f32)]
    work = pl.pallas_call(
        functools.partial(prepare, regions, packed),
        out_shape=[
            shape((2 * LANES, 2 * LANES), bf16),
            shape((half, 4 * rows, LANES), f32),
            shape((half * rows, 2 * LANES), f32),
            shape((regions, 2 * depth, LANES), f32),
            shape((2 * depth, LANES), f32),
        ],
        in_specs=[vmem] * 2,
        out_specs=[vmem] * 5,
        scratch_shapes=[pltpu.VMEM((half, 2 * (rows + HALO), LANES), f32)]
        + scratch[:3]
        + [pltpu.VMEM((2 * LANES, 2 * LANES), bf16)],
        compiler_params=limit,
        cost_estimate=pl.CostEstimate(flops=400_000_000, bytes_accessed=2_000_000, transcendentals=0),
        name="prepare",
    )
    near, far = matchings(row_count)
    first = lax.ppermute(sent[0], "row", near)

    def edge(contrast, x):
        return x, *work(contrast, starts)

    def inner(contrast, x):
        x = lax.ppermute(x, "row", far)
        return x, *work(contrast, starts)

    row = lax.axis_index("row")
    second, *ready = lax.cond((row == 0) | (row == row_count - 1), edge, inner, contrast, sent[1])
    cut = pl.pallas_call(
        functools.partial(chain, regions, packed),
        out_shape=[shape((rows, LANES), bf16)] * regions if packed else [shape((regions, rows, LANES), bf16)],
        in_specs=[vmem] * 7,
        out_specs=[vmem] * (regions if packed else 1),
        scratch_shapes=scratch,
        compiler_params=limit,
        name="chain",
    )(first, second, *ready)
    if packed:
        mine = [cut[0]]
        for i in range(1, regions):
            mine.append(lax.ppermute(cut[i], "ang", list(enumerate(rounds(regions)[i]))))
    else:
        mine = [lax.all_to_all(cut[0], "ang", 0, 0, tiled=True)]
    placed = pl.pallas_call(
        functools.partial(place, angles, packed),
        out_shape=shape((angles * LANES, pixels), bf16),
        in_specs=[pl.BlockSpec(memory_space=pltpu.SMEM), vmem],
        out_specs=vmem,
        compiler_params=limit,
        cost_estimate=pl.CostEstimate(flops=100_000_000, bytes_accessed=400_000, transcendentals=0),
        name="place",
    )(block_start, bp_weights)
    return pl.pallas_call(
        functools.partial(finish, angles, packed),
        out_shape=shape((rows, pixels), f32),
        in_specs=[vmem] * (len(mine) + 1),
        out_specs=vmem,
        compiler_params=limit,
        name="finish",
    )(*mine, placed)


def solution(mesh):
    placed = (P(("scan", "ang"), "row", None), P(("scan", "row"), None), P(), P(None, None, "ang"))
    return jax.shard_map(body, mesh=mesh, in_specs=placed, out_specs=P(("scan", "row"), "ang"), check_vma=False)
```

```python
import functools

import jax
import jax.numpy as jnp
import numpy as np
from jax import lax
from jax.experimental import pallas as pl
from jax.experimental.pallas import tpu as pltpu
from jax.sharding import PartitionSpec as P


HALO = 4
LANES = 128
RING = (0, 2, 1, 3)
LAST = 2
FIRST = (0, 1, 3)
paganin_beta = 8.0
ramp_gain = 320.0


def split(x):
    high = x.astype(jnp.bfloat16)
    low = (x - high.astype(jnp.float32)).astype(jnp.bfloat16)
    return high, low


def sizes(width, rows):
    blocks = width // LANES
    half = blocks // 2 + 1
    return blocks, half, half + -half % 8, rows + 2 * HALO


def wave(j, period):
    y = (2 * j - period).astype(jnp.float32) * np.float32(np.pi / (2 * period))
    z = y * y
    p = np.float32(-1 / 39916800)
    for c in (1 / 362880, -1 / 5040, 1 / 120, -1 / 6, 1.0):
        p = p * z + np.float32(c)
    y = y * p
    return 2.0 * y * y - 1.0


def late(j, period):
    return jnp.where(j >= period // 4, j - period // 4, j + period - period // 4)


def iotas(rows, lanes=LANES):
    return (lax.broadcasted_iota(jnp.int32, (rows, lanes), d) for d in (0, 1))


def matrices(m_high, m_low):
    row, col = iotas(LANES)
    c, s = wave(row * col & (LANES - 1), LANES), wave((row * col - LANES // 4) & (LANES - 1), LANES)
    for ref, c, s in zip((m_high, m_low), split(c), split(s)):
        ref[:LANES, :LANES], ref[:LANES, LANES:] = c, -s
        ref[LANES:, :LANES], ref[LANES:, LANES:] = s, c


def real_dft(x):
    n = len(x)
    h = n // 2
    plus = {a: x[a] + x[n - a] for a in range(1, h)}
    minus = {a: x[a] - x[n - a] for a in range(1, h)}
    re, im = [None] * (h + 1), [None] * (h + 1)

    def total(terms):
        acc = None
        for c, y in terms:
            if abs(c) < 1e-12:
                continue
            z = y if c == 1.0 else (-y if c == -1.0 else y * np.float32(c))
            acc = z if acc is None else acc + z
        return acc

    def cos(m):
        return float(np.round(np.cos(2 * np.pi * (m % n) / n), 15))

    def sin(m):
        return float(np.round(np.sin(2 * np.pi * (m % n) / n), 15))

    for k in range(h // 2 + 1):
        ends = {0: x[0], h: x[h]}
        even = total([(cos(a * k), ends.get(a, plus.get(a))) for a in range(0, h + 1, 2)])
        odd = total([(cos(a * k), ends.get(a, plus.get(a))) for a in range(1, h + 1, 2)])
        re[k] = even if odd is None else even + odd
        re[h - k] = even if odd is None else even - odd
        even = total([(sin(a * k), minus[a]) for a in range(2, h, 2)])
        odd = total([(sin(a * k), minus[a]) for a in range(1, h, 2)])
        parts = [y for y in (even, odd) if y is not None]
        if parts:
            im[k] = -parts[0] if len(parts) == 1 else -(even + odd)
            if h - k != k:
                im[h - k] = (even - odd) if len(parts) == 2 else (even if odd is None else -odd)
    return re, im


def product(passes, high, low, x, m_high, m_low, turned):
    dims = (((1,), (1 if turned else 0,)), ((), ()))
    dot = functools.partial(lax.dot_general, dimension_numbers=dims, preferred_element_type=jnp.float32)
    n = x[0].shape[0]
    for k, part in enumerate(x):
        at = slice(k * n, (k + 1) * n)
        if passes == 1:
            high[at, :] = part.astype(jnp.bfloat16)
        else:
            high[at, :], low[at, :] = split(part)
    out = dot(high[...], m_high)
    if passes > 1:
        out += dot(low[...], m_high)
    if passes > 2:
        out += dot(high[...], m_low)
    return out


def filtered(passes, x, begins, m_high, m_low, kern, turn, high, low, spec):
    rows, blocks = x[0].shape[0], len(x)
    _, half, depth, _ = sizes(blocks * LANES, rows)
    m_high, m_low = m_high[...], m_low[...] if passes > 2 else None
    re, im = real_dft(x)
    parts = []
    for k in range(half):
        c, s = turn[k : k + 1], turn[depth + k : depth + k + 1]
        if im[k] is None:
            parts.append(jnp.concatenate([re[k] * c, -re[k] * s], axis=1))
        else:
            parts.append(jnp.concatenate([re[k] * c + im[k] * s, im[k] * c - re[k] * s], axis=1))
    whole = product(passes, high, low, parts, m_high, m_low, False)
    spec[...] = whole
    parts = []
    for k in range(half):
        re = im = None
        for t, begin in enumerate(begins):
            entry = kern[k, pl.ds(begin, rows), :]
            row = k * rows + t
            a, b = entry * whole[row : row + 1, :LANES], entry * spec[row : row + 1, LANES:]
            re, im = (a, b) if re is None else (re + a, im + b)
        parts.append(jnp.concatenate([re, im], axis=1))
    return product(passes, high, low, parts, m_high, m_low, True)


def begin(proj_in, flats_in, starts_in, own, first, second, starts, proj, flats, sems):
    rows, width = own.shape
    pieces = sems.shape[0] // 2
    step = width // pieces
    late = pltpu.make_async_copy(starts_in, starts, sems.at[2 * pieces])
    copies = []
    for i in range(pieces):
        at = pl.ds(i * step, step)
        copies.append(pltpu.make_async_copy(flats_in.at[:, at], flats.at[:, at], sems.at[2 * i]))
        copies.append(pltpu.make_async_copy(proj_in.at[0, :, at], proj.at[:, at], sems.at[2 * i + 1]))
    for k, copy in enumerate((*copies, late)):
        copy.start(priority=k % 2)
    even = lax.rem(lax.axis_index("row"), 2) == 0
    for i in range(pieces):
        copies[2 * i].wait()
        copies[2 * i + 1].wait()
        at = slice(i * step, (i + 1) * step)
        contrast = 1.0 - proj[:, at].astype(jnp.float32) / flats[:, at]
        own[:, at] = contrast
        initial, last = contrast[:HALO], contrast[rows - HALO :]
        first[:, at] = jnp.where(even, last, initial).astype(first.dtype)
        second[:, at] = jnp.where(even, initial, last).astype(second.dtype)
    late.wait()


def each(count, packed, f):
    if packed:
        for i in range(count):
            f(i)
    else:
        pl.loop(0, count)(f)


def prepare(regions, packed, own, starts, m_high, near, back, phases, turn, kern, high, low, spec, m_low):
    rows, width = own.shape
    blocks, half, depth, tile = sizes(width, rows)
    spread = rows + HALO
    matrices(m_high, m_low)
    k, lane = iotas(depth)
    turn[:depth, :], turn[depth:, :] = wave(k * lane, width), wave(late(k * lane, width), width)
    around = lax.rem(k * lane, blocks)
    jump = jnp.concatenate([wave(around, blocks), wave(lax.rem(around + blocks - blocks // 4, blocks), blocks)], axis=0)
    v = k + blocks * lane
    folded = jnp.minimum(v, width - v)
    part = jnp.where((k == 0) | (2 * k == blocks), 1.0 / width, 2.0 / width)
    folded_wave = wave(folded, width)
    gain = ramp_gain * (folded.astype(jnp.float32) / width) * (0.5 + 0.5 * folded_wave) * part
    across = 1.0 + paganin_beta * (2.0 - 2.0 * folded_wave)
    u, _ = iotas(tile)
    along = paganin_beta * (2.0 - 2.0 * wave(u, tile))
    parts = [gain[k : k + 1] / (along + across[k : k + 1]) for k in range(half)]
    f_high, f_low = split(jnp.concatenate(parts, axis=1))
    i, u = iotas(2 * spread, tile)
    count = jnp.where(2 * u > tile, 0.0, jnp.where((u == 0) | (2 * u == tile), 1.0 / tile, 2.0 / tile))
    mix_high, mix_low = split(count * wave(lax.rem((i + tile * spread - spread) * u, tile), tile))
    dot = functools.partial(jnp.dot, preferred_element_type=jnp.float32)
    entries = dot(mix_high, f_high) + dot(mix_high, f_low) + dot(mix_low, f_high)
    row, me = lax.axis_index("row"), lax.axis_index("ang")
    even = lax.rem(row, 2) == 0
    inside = (row > 0) & (row < lax.axis_size("row") - 1)
    reach = rows + HALO - 1
    for k in range(half):
        kern[k] = entries[:, k * LANES : (k + 1) * LANES]
        below, above = kern[k, 1 : 1 + reach, :], kern[k, 2 * spread - reach : 2 * spread, :]
        near[k, :reach, :] = jnp.where(even, below, above)
        near[k, 2 * rows : 2 * rows + reach, :] = jnp.where(inside, jnp.where(even, above, below), 0.0)
    lanes = lax.broadcasted_iota(jnp.int32, (1, LANES), 1).astype(jnp.float32)
    angle, column = iotas(*starts.shape)
    mine = jnp.where(angle == me, starts[...].astype(jnp.float32), 0.0)
    c, s = turn[:depth, :], turn[depth:, :]

    def phase(i):
        start = jnp.where(column == (target(me, i, regions) if packed else i), mine, 0.0)
        start = jnp.sum(jnp.sum(start, axis=1, keepdims=True), axis=0, keepdims=True)
        block = jnp.floor(start * (1.0 / LANES))
        here, after = (jnp.sum(jnp.where(lanes == b, jump, 0.0), axis=1, keepdims=True) for b in (block, block + 1.0))
        far = jnp.where(lanes >= start - LANES * block, here, after)
        fc, fs = far[:depth], far[depth:]
        phases[i] = jnp.concatenate([c * fc - s * fs, -(s * fc + c * fs)], axis=0)

    each(regions, packed, phase)
    x = [own[:, LANES * a : LANES * (a + 1)] for a in range(blocks)]
    back[...] = filtered(3, x, [spread - t for t in range(rows)], m_high, m_low, kern, turn, high, low, spec)


def chain(regions, packed, first, second, m_high, near, own_back, phases, turn, *rest):
    outs, (high, low, spec, back) = rest[:-4], rest[-4:]
    width, rows = first.shape[1], near.shape[1] // 4
    blocks, half, depth, _ = sizes(width, rows)
    x = jnp.concatenate([first[...].astype(jnp.float32), second[...].astype(jnp.float32)], axis=0)
    begins = [begin + HALO - 1 - t for begin in (0, 2 * rows) for t in range(HALO)]
    x = [x[:, LANES * a : LANES * (a + 1)] for a in range(blocks)]
    back[...] = filtered(PASSES, x, begins, m_high, None, near, turn, high, low, spec) + own_back[...]

    def region(i):
        value = None
        for k in range(half):
            v = back[k * rows : (k + 1) * rows, :]
            term = v[:, :LANES] * phases[i, k : k + 1, :] + v[:, LANES:] * phases[i, depth + k : depth + k + 1, :]
            value = term if value is None else value + term
        if packed:
            outs[i][...] = value.astype(jnp.bfloat16)
        else:
            outs[0][i] = value.astype(jnp.bfloat16)

    each(regions, packed, region)


PASSES = 1
PIECES = 2


def place(angles, packed, starts, weights, placed):
    cb = weights.shape[1]
    me = lax.axis_index("ang")

    def one(i):
        a = source(me, i, angles) if packed else i
        offset = lax.rem(starts[a, me], LANES)
        spot = lax.broadcasted_iota(jnp.int32, (LANES, cb), 0) - lax.broadcasted_iota(jnp.int32, (LANES, cb), 1)
        spot = ((spot == offset) | (spot == offset - LANES)).astype(jnp.float32).astype(jnp.bfloat16)
        value = jnp.dot(spot, weights[a], preferred_element_type=jnp.float32).astype(placed.dtype)
        placed[pl.ds(pl.multiple_of(i * LANES, LANES), LANES) if not packed else pl.ds(i * LANES, LANES), :] = value

    each(angles, packed, one)


def partial(*refs):
    *cut, placed, out = refs
    total = None
    for i, x in zip(FIRST, cut):
        term = jnp.dot(x[...], placed[i * LANES : (i + 1) * LANES, :], preferred_element_type=jnp.float32)
        total = term if total is None else total + term
    out[...] = total


def finish(blocks, packed, *refs):
    *cut, placed, out = refs
    dot = functools.partial(jnp.dot, preferred_element_type=jnp.float32)
    if packed:
        last, part = cut
        out[...] = part[...] + dot(last[...], placed[LAST * LANES : (LAST + 1) * LANES, :])
    else:
        out[...] = jnp.zeros_like(out)

        @pl.loop(0, blocks)
        def _(a):
            out[...] += dot(cut[0][a], placed[pl.ds(pl.multiple_of(a * LANES, LANES), LANES), :])


def rounds(count):
    ring = RING if count == len(RING) else range(count)
    place = {x: p for p, x in enumerate(ring)}
    return [[ring[(place[x] + i) % count] for x in range(count)] for i in range(count)]


def pick(me, values):
    out = jnp.int32(0)
    for x, y in enumerate(values):
        out = jnp.where(me == x, y, out)
    return out


def target(me, i, count):
    return pick(me, rounds(count)[i])


def source(me, i, count):
    return pick(me, rounds(count)[-i % count])


def matchings(count):
    for start in (0, 1):
        ends = [(i, i + 1) for i in range(start, count - 1, 2)]
        if start and count % 2 == 0:
            ends.append((count - 1, 0))
        yield [pair for i, j in ends for pair in ((i, j), (j, i))]


def body(projections, flats, block_start, bp_weights):
    _, rows, width = projections.shape
    angles, _, pixels = bp_weights.shape
    regions, row_count = lax.axis_size("ang"), lax.axis_size("row")
    _, half, depth, _ = sizes(width, rows)
    f32, bf16 = jnp.float32, jnp.bfloat16
    shape = jax.ShapeDtypeStruct
    vmem = pl.BlockSpec(memory_space=pltpu.VMEM)
    limit = pltpu.CompilerParams(vmem_limit_bytes=12 * 1024 * 1024)
    packing = pltpu.CompilerParams(vmem_limit_bytes=12 * 1024 * 1024)
    packed = regions == len(RING)
    pieces = PIECES if width % (PIECES * LANES) == 0 else 1
    hbm = pl.BlockSpec(memory_space=pltpu.HBM)
    contrast, *sent, starts = pl.pallas_call(
        begin,
        out_shape=[shape((rows, width), f32)] + [shape((HALO, width), bf16)] * 2 + [shape(block_start.shape, block_start.dtype)],
        in_specs=[hbm] * 3,
        out_specs=[vmem] * 4,
        scratch_shapes=[
            pltpu.VMEM((rows, width), bf16),
            pltpu.VMEM((rows, width), f32),
            pltpu.SemaphoreType.DMA((2 * pieces + 1,)),
        ],
        compiler_params=limit,
        name="begin",
    )(*(pltpu.with_memory_space_constraint(x, pltpu.HBM) for x in (projections, flats, block_start)))
    scratch = [pltpu.VMEM((half * rows, 2 * LANES), t) for t in (bf16, bf16, f32, f32)]
    work = pl.pallas_call(
        functools.partial(prepare, regions, packed),
        out_shape=[
            shape((2 * LANES, 2 * LANES), bf16),
            shape((half, 4 * rows, LANES), f32),
            shape((half * rows, 2 * LANES), f32),
            shape((regions, 2 * depth, LANES), f32),
            shape((2 * depth, LANES), f32),
        ],
        in_specs=[vmem] * 2,
        out_specs=[vmem] * 5,
        scratch_shapes=[pltpu.VMEM((half, 2 * (rows + HALO), LANES), f32)]
        + scratch[:3]
        + [pltpu.VMEM((2 * LANES, 2 * LANES), bf16)],
        compiler_params=packing,
        cost_estimate=pl.CostEstimate(flops=400_000_000, bytes_accessed=2_000_000, transcendentals=0),
        name="prepare",
    )
    near, far = matchings(row_count)
    first = lax.ppermute(sent[0], "row", near)

    def edge(contrast, x):
        return x, *work(contrast, starts)

    def inner(contrast, x):
        x = lax.ppermute(x, "row", far)
        return x, *work(contrast, starts)

    row = lax.axis_index("row")
    second, *ready = lax.cond((row == 0) | (row == row_count - 1), edge, inner, contrast, sent[1])
    cut = pl.pallas_call(
        functools.partial(chain, regions, packed),
        out_shape=[shape((rows, LANES), bf16)] * regions if packed else [shape((regions, rows, LANES), bf16)],
        in_specs=[vmem] * 7,
        out_specs=[vmem] * (regions if packed else 1),
        scratch_shapes=scratch,
        compiler_params=packing,
        name="chain",
    )(first, second, *ready)
    if packed:
        mine = [cut[0]]
        for i in range(1, regions):
            mine.append(lax.ppermute(cut[i], "ang", list(enumerate(rounds(regions)[i]))))
    else:
        mine = [lax.all_to_all(cut[0], "ang", 0, 0, tiled=True)]
    placed = pl.pallas_call(
        functools.partial(place, angles, packed),
        out_shape=shape((angles * LANES, pixels), bf16),
        in_specs=[pl.BlockSpec(memory_space=pltpu.SMEM), vmem],
        out_specs=vmem,
        compiler_params=limit,
        cost_estimate=pl.CostEstimate(flops=100_000_000, bytes_accessed=400_000, transcendentals=0),
        name="place",
    )(block_start, bp_weights)
    if packed:
        part = pl.pallas_call(
            partial,
            out_shape=shape((rows, pixels), f32),
            in_specs=[vmem] * (len(FIRST) + 1),
            out_specs=vmem,
            compiler_params=limit,
            name="partial",
        )(*(mine[i] for i in FIRST), placed)
        mine = [mine[LAST], part]
    return pl.pallas_call(
        functools.partial(finish, angles, packed),
        out_shape=shape((rows, pixels), f32),
        in_specs=[vmem] * (len(mine) + 1),
        out_specs=vmem,
        compiler_params=limit,
        name="finish",
    )(*mine, placed)


def solution(mesh):
    placed = (P(("scan", "ang"), "row", None), P(("scan", "row"), None), P(), P(None, None, "ang"))
    return jax.shard_map(body, mesh=mesh, in_specs=placed, out_specs=P(("scan", "row"), "ang"), check_vma=False)
```
